32 devices in a mesh: grp: 4 (over z), shard: 8 (over y, x, core).
Axes of the slice: x: 2, y: 2, z: 4, core: 2. Of those that a mesh axis runs over, the one named last changes fastest.
Arguments:
- partial_grads: bfloat16 [4, 4096, 6144], P('grp', 'shard')
- joined_block: int32 [48], replicated, may hold values from 0 to 47, each once
- head_slot: int32 [48], replicated, may hold values from 0 to 47, as said below
Outputs:
- head_grads: float32 [48, 8, 512, 128], P('shard', None, 'grp')
- head_rms: float32 [48], P('shard')
- type_rms: float32 [3], replicated
The draws below stay inside these ranges and needn't reach their ends.
Inputs may be any that keep to these rules, and one draw needn't show every extreme that they name: `joined_block`: a permutation: each block number appears once. `head_slot`: distinct slots; every owner along shard holds 6 or 5 head blocks, and some owner holds 6.
All inputs are finite; a program needn't handle non-finite values.
Results may differ from the reference program's by a relative error of at most 0.0003.
Values may be sent and summed in bfloat16 or wider, within the bound.
A program may use at most 64 MiB of HBM per device.

```python
import jax
import jax.numpy as jnp
from jax import lax

D = 4096
QH = 32
KVH = 8
HS = 128
BLOCKS = 48
COLS = 6144
SLOTS_DEV = 6
SLOTS = 48
N_GRP = 4
N_SHARD = 8


def draw_partial_grads(key, part):
    row_index = jnp.arange(D)
    block_pos = (row_index % (D // N_SHARD)).astype(jnp.float32) / (D // N_SHARD)
    rise = jnp.exp(jnp.log(3.0) * block_pos)
    row_scale = jnp.exp(jax.random.uniform(jax.random.fold_in(key, 11), (D,), jnp.float32, 0.0, jnp.log(10.0))) * rise
    col_scale = jnp.exp(jax.random.uniform(jax.random.fold_in(key, 12), (COLS,), jnp.float32, 0.0, jnp.log(10.0)))
    overall = 0.01

    def draw_group(group):
        noise = jax.random.normal(jax.random.fold_in(jax.random.fold_in(key, 14), group), (D, COLS), jnp.float32)
        return (noise * row_scale[:, None] * col_scale[None, :] * overall).astype(jnp.bfloat16)
    return lax.map(draw_group, jnp.arange(N_GRP))


def draw_head_slot(key, part):
    slot_total = SLOTS_DEV * N_SHARD
    empty_count = slot_total - BLOCKS
    owners = jax.random.permutation(jax.random.fold_in(key, 21), N_SHARD).astype(jnp.int32)
    lost_pos = jax.random.randint(jax.random.fold_in(key, 22), (N_SHARD,), 0, SLOTS_DEV).astype(jnp.int32)
    lost_slot = owners * SLOTS_DEV + lost_pos
    chosen = jnp.arange(N_SHARD, dtype=jnp.int32) < empty_count
    slot_ids = jnp.arange(slot_total, dtype=jnp.int32)
    dead_slot = jnp.any((slot_ids[:, None] == lost_slot[None, :]) & chosen[None, :], axis=1)
    sort_keys = dead_slot.astype(jnp.int32) * slot_total + slot_ids
    live_slots = jnp.argsort(sort_keys).astype(jnp.int32)[:BLOCKS]
    shuffle = jax.random.permutation(jax.random.fold_in(key, 23), BLOCKS).astype(jnp.int32)
    return live_slots[shuffle].astype(jnp.int32)


def setup_inputs(seed: int = 0) -> dict:
    streams_of = jax.random.split(jax.random.key(seed), 4)
    return {
        "partial_grads": draw_partial_grads(jax.random.fold_in(streams_of[3], 71), 0),
        "joined_block": jax.random.permutation(streams_of[1], BLOCKS).astype(jnp.int32),
        "head_slot": draw_head_slot(jax.random.fold_in(streams_of[3], 71), 0),
    }


def reference(partial_grads, joined_block, head_slot):

    def add_group(carry, group_term):
        return (carry + group_term.astype(jnp.float32), None)
    reduced, _ = lax.scan(add_group, jnp.zeros((D, COLS), jnp.float32), partial_grads)
    block_ids = jnp.arange(BLOCKS, dtype=jnp.int32)
    block_kind = (block_ids >= QH).astype(jnp.int32) + (block_ids >= QH + KVH).astype(jnp.int32)
    matches = (head_slot[None, :] == jnp.arange(SLOTS, dtype=jnp.int32)[:, None]).astype(jnp.int32)
    occupied = lax.optimization_barrier(jnp.sum(matches, axis=1))
    source = lax.optimization_barrier(jnp.sum(matches * joined_block[None, :], axis=1)).astype(jnp.int32)
    slot_kind = lax.optimization_barrier(jnp.sum(matches * block_kind[None, :], axis=1)) + (1 - occupied) * 3
    picked = jnp.take(reduced.reshape(D, BLOCKS, HS), source, axis=1)
    picked = picked * occupied.astype(jnp.float32)[None, :, None]
    head_grads = jnp.transpose(picked, (1, 0, 2)).reshape(SLOTS, N_SHARD, D // N_SHARD, HS)
    squares = lax.optimization_barrier(jnp.sum(head_grads * head_grads, axis=(1, 2, 3)))
    head_rms = jnp.sqrt(squares / (D * HS))
    selector = (slot_kind[:, None] == jnp.arange(3, dtype=jnp.int32)[None, :]).astype(jnp.float32)
    type_squares = lax.optimization_barrier(jnp.sum(squares[:, None] * selector, axis=0))
    counts = jnp.array([QH, KVH, KVH], jnp.float32) * (D * HS)
    type_rms = jnp.sqrt(type_squares / counts)
    return (head_grads, head_rms, type_rms)
```

```python
import functools

import jax
import jax.numpy as jnp
from jax import lax
from jax.experimental import pallas as pl
from jax.experimental.pallas import tpu as pltpu
from jax.sharding import PartitionSpec as P

D = 4096
QH = 32
KVH = 8
HS = 128
LANES = 128
MESH = pl.DeviceIdType.MESH


def chunk_rows(rows):
    return 16 if rows % 16 == 0 else rows


def kernel(groups, shards, blocks, slots_dev, chunks, *refs):
    x_ref, joined_ref, slot_ref = refs[:3]
    out_ref, head_ref, type_ref = refs[3:6]
    own = refs[6]
    got = refs[7 : 7 + chunks]
    ready = refs[7 + chunks : 7 + 2 * chunks]
    rest = refs[7 + 2 * chunks :]
    (source, taken, kind_of, summed, squares, shard_part, shard_all, grp_part, grp_all) = rest[:9]
    (own_sem, z_send, z_recv, a_send, a_recv, keep_sem, s_send, s_recv, g_send, g_recv) = rest[9:]

    grp = lax.axis_index("grp")
    shard = lax.axis_index("shard")
    slots = slots_dev * shards
    rows = own.shape[0]
    part = rows // chunks
    width = own.shape[1] // blocks

    def grp_peer(offset):
        return lax.rem(grp + offset, groups)

    def shard_peer(offset):
        return lax.rem(shard + offset, shards)

    load_own = pltpu.make_async_copy(
        x_ref.at[0, pl.ds(pl.multiple_of(grp * rows, 8), rows), :], own, own_sem
    )
    load_own.start()

    barrier = pltpu.get_barrier_semaphore()
    for o in range(1, groups):
        pl.semaphore_signal(barrier, 1, device_id=(grp_peer(o), shard), device_id_type=MESH)
    for o in range(1, shards):
        pl.semaphore_signal(barrier, 1, device_id=(grp, shard_peer(o)), device_id_type=MESH)
    pl.semaphore_wait(barrier, groups + shards - 2)

    z_copies = []
    for c in range(chunks):
        for o in range(1, groups):
            first = pl.multiple_of(grp_peer(o) * rows + c * part, 8)
            copy = pltpu.make_async_remote_copy(
                src_ref=x_ref.at[0, pl.ds(first, part), :],
                dst_ref=got[c].at[o - 1],
                send_sem=z_send.at[c, o - 1],
                recv_sem=z_recv.at[c, o - 1],
                device_id=(grp_peer(o), shard),
                device_id_type=MESH,
            )
            copy.start()
            z_copies.append(copy)

    def find(j, carry):
        found, block, kind = jnp.float32(0), jnp.int32(0), jnp.int32(3)
        for b in range(blocks):
            hit = slot_ref[b] == j
            found = jnp.where(hit, 1.0, found)
            block = jnp.where(hit, joined_ref[b], block)
            kind = jnp.where(hit, (b >= QH) + (b >= QH + KVH), kind)
        source[j] = block
        taken[j] = found
        kind_of[j] = kind
        return carry

    lax.fori_loop(0, slots, find, 0)

    load_own.wait()
    a_copies = []
    for c in range(chunks):
        for o in range(1, groups):
            z_copies[c * (groups - 1) + o - 1].wait_recv()

        def add(k, carry):
            at = pl.multiple_of(k * width, width)
            total = own[c * part : (c + 1) * part, pl.ds(at, width)].astype(jnp.float32)
            for o in range(1, groups):
                total += got[c][o - 1, :, pl.ds(at, width)].astype(jnp.float32)
            summed[k] = total
            return carry

        lax.fori_loop(0, blocks, add, 0, unroll=4)

        def slot(j, carry):
            total = summed[source[j]] * taken[j]
            ready[c][j] = total
            sq = jnp.sum((total * total).reshape(part // 8, 8, width), axis=0)
            squares[j] = sq if c == 0 else squares[j] + sq
            return carry

        lax.fori_loop(0, slots, slot, 0, unroll=4)

        if c == chunks - 1:
            lane = lax.broadcasted_iota(jnp.int32, (slots, LANES), 1)
            row = lax.broadcasted_iota(jnp.int32, (slots, LANES), 0)
            per_slot = jnp.sum(jnp.sum(squares[...], axis=1), axis=1, keepdims=True)
            shard_part[...] = jnp.sum(jnp.where(lane == row, per_slot, 0.0), axis=0, keepdims=True)
            s_copies = []
            for o in range(1, shards):
                copy = pltpu.make_async_remote_copy(
                    src_ref=shard_part,
                    dst_ref=shard_all.at[o - 1],
                    send_sem=s_send.at[o - 1],
                    recv_sem=s_recv.at[o - 1],
                    device_id=(grp, shard_peer(o)),
                    device_id_type=MESH,
                )
                copy.start()
                s_copies.append(copy)

        for o in range(1, shards):
            copy = pltpu.make_async_remote_copy(
                src_ref=ready[c].at[pl.ds(shard_peer(o) * slots_dev, slots_dev)],
                dst_ref=out_ref.at[:, shard, pl.ds(c * part, part), :],
                send_sem=a_send.at[c, o - 1],
                recv_sem=a_recv.at[c, o - 1],
                device_id=(grp, shard_peer(o)),
                device_id_type=MESH,
            )
            copy.start()
            a_copies.append(copy)
        copy = pltpu.make_async_copy(
            ready[c].at[pl.ds(shard * slots_dev, slots_dev)],
            out_ref.at[:, shard, pl.ds(c * part, part), :],
            keep_sem.at[c],
        )
        copy.start()
        a_copies.append(copy)

    total = shard_part[...]
    for o in range(1, shards):
        s_copies[o - 1].wait()
        total = total + shard_all[o - 1]
    grp_part[...] = total
    g_copies = []
    for o in range(1, groups):
        copy = pltpu.make_async_remote_copy(
            src_ref=grp_part,
            dst_ref=grp_all.at[o - 1],
            send_sem=g_send.at[o - 1],
            recv_sem=g_recv.at[o - 1],
            device_id=(grp_peer(o), shard),
            device_id_type=MESH,
        )
        copy.start()
        g_copies.append(copy)
    lane = lax.broadcasted_iota(jnp.int32, (1, LANES), 1)

    def lay(j, kinds):
        return jnp.where(lane == j, kind_of[j], kinds)

    kinds = lax.fori_loop(0, slots, lay, jnp.full((1, LANES), 3, jnp.int32))
    for o in range(1, groups):
        g_copies[o - 1].wait()
        total = total + grp_all[o - 1]
    root = jnp.sqrt(total / (D * HS))
    for i in range(slots_dev):
        head_ref[i] = jnp.sum(jnp.where(lane == shard * slots_dev + i, root, 0.0))
    for t, heads in enumerate((QH, KVH, KVH)):
        one = jnp.sum(jnp.where(kinds == t, total, 0.0), axis=1, keepdims=True)
        type_ref[t] = jnp.sum(jnp.sqrt(one / (heads * D * HS)))

    for copy in z_copies:
        copy.wait_send()
    for copy in a_copies:
        copy.wait()


def solution(mesh):
    groups, shards = mesh.shape["grp"], mesh.shape["shard"]

    def step(x, joined, slot):
        blocks = joined.shape[0]
        slots_dev = (blocks + shards - 1) // shards
        slots = slots_dev * shards
        rows = x.shape[1] // groups
        cols = x.shape[2]
        width = cols // blocks
        part = chunk_rows(rows)
        chunks = rows // part
        dma = pltpu.SemaphoreType.DMA
        return tuple(
            pl.pallas_call(
                functools.partial(kernel, groups, shards, blocks, slots_dev, chunks),
                out_shape=[
                    jax.ShapeDtypeStruct((slots_dev, shards, rows, width), jnp.float32),
                    jax.ShapeDtypeStruct((slots_dev,), jnp.float32),
                    jax.ShapeDtypeStruct((3,), jnp.float32),
                ],
                in_specs=[
                    pl.BlockSpec(memory_space=pl.ANY),
                    pl.BlockSpec(memory_space=pltpu.SMEM),
                    pl.BlockSpec(memory_space=pltpu.SMEM),
                ],
                out_specs=[
                    pl.BlockSpec(memory_space=pl.ANY),
                    pl.BlockSpec(memory_space=pltpu.SMEM),
                    pl.BlockSpec(memory_space=pltpu.SMEM),
                ],
                scratch_shapes=[pltpu.VMEM((rows, cols), jnp.bfloat16)]
                + [pltpu.VMEM((groups - 1, part, cols), jnp.bfloat16)] * chunks
                + [pltpu.VMEM((slots, part, width), jnp.float32)] * chunks
                + [
                    pltpu.SMEM((slots,), jnp.int32),
                    pltpu.SMEM((slots,), jnp.float32),
                    pltpu.SMEM((slots,), jnp.int32),
                    pltpu.VMEM((blocks, part, width), jnp.float32),
                    pltpu.VMEM((slots, 8, width), jnp.float32),
                    pltpu.VMEM((1, LANES), jnp.float32),
                    pltpu.VMEM((shards - 1, 1, LANES), jnp.float32),
                    pltpu.VMEM((1, LANES), jnp.float32),
                    pltpu.VMEM((groups - 1, 1, LANES), jnp.float32),
                    dma,
                    dma((chunks, groups - 1)),
                    dma((chunks, groups - 1)),
                    dma((chunks, shards - 1)),
                    dma((chunks, shards - 1)),
                    dma((chunks,)),
                    dma((shards - 1,)),
                    dma((shards - 1,)),
                    dma((groups - 1,)),
                    dma((groups - 1,)),
                ],
                compiler_params=pltpu.CompilerParams(
                    collective_id=0,
                    has_side_effects=True,
                    vmem_limit_bytes=60 * 1024 * 1024,
                ),
            )(x, joined, slot)
        )

    return jax.shard_map(
        step,
        mesh=mesh,
        in_specs=(P("grp", "shard", None), P(), P()),
        out_specs=(P("shard", None, "grp", None), P("shard"), P()),
        check_vma=False,
    )
```

```python
import functools

import jax
import jax.numpy as jnp
from jax import lax
from jax.experimental import pallas as pl
from jax.experimental.pallas import tpu as pltpu
from jax.sharding import PartitionSpec as P

D = 4096
QH = 32
KVH = 8
HS = 128
LANES = 128
MESH = pl.DeviceIdType.MESH


def chunk_rows(rows):
    return 16 if rows % 16 == 0 else rows


QMAX = 8388600.0
TINY = 2.0**-126


def pack(pair):
    peaks, codes = [], []
    for tile in pair:
        peak = jnp.max(jnp.abs(tile), axis=(0, 1), keepdims=True)
        shrink = jnp.where(peak > 2.0**100, 2.0**-24, 1.0)
        scale = 1.0 / jnp.maximum(peak * shrink, TINY)
        code = jnp.round(tile * shrink * scale * QMAX).astype(jnp.int32)
        peaks.append(peak)
        codes += [code[:8], code[8:]]
    a, b, c, d = codes
    words = (
        (a << 8) | (d & 255),
        (b << 8) | ((d >> 8) & 255),
        (c << 8) | ((d >> 16) & 255),
    )
    return words, peaks


def unpack(words):
    a, b, c = words
    d = (a & 255) | ((b & 255) << 8) | ((c << 24) >> 8)
    return [
        jnp.concatenate([lo.astype(jnp.float32), hi.astype(jnp.float32)], axis=0) * (1.0 / QMAX)
        for lo, hi in ((a >> 8, b >> 8), (c >> 8, d))
    ]


def kernel(groups, shards, blocks, slots_dev, chunks, relay, *refs):
    x_ref, joined_ref, slot_ref = refs[:3]
    out_ref, head_ref, type_ref = refs[3:6]
    own = refs[6]
    got = refs[7 : 7 + chunks]
    ready = refs[7 + chunks : 7 + 2 * chunks]
    rest = refs[7 + 2 * chunks :]
    if relay:
        far, passed, out_words, out_peaks, in_words, in_peaks = rest[-11:-5]
        far_sem, r_send, r_recv, p_send, p_recv = rest[-5:]
        rest = rest[:-11]
    (source, taken, kind_of, summed, squares, shard_part, shard_all, grp_part, grp_all) = rest[:9]
    (own_sem, z_send, z_recv, a_send, a_recv, keep_sem, s_send, s_recv, g_send, g_recv) = rest[9:]

    grp = lax.axis_index("grp")
    shard = lax.axis_index("shard")
    slots = slots_dev * shards
    rows = own.shape[0]
    part = rows // chunks
    width = own.shape[1] // blocks

    def grp_peer(offset):
        return lax.rem(grp + offset, groups)

    def shard_peer(offset):
        return lax.rem(shard + offset, shards)

    load_own = pltpu.make_async_copy(
        x_ref.at[0, pl.ds(pl.multiple_of(grp * rows, 8), rows), :], own, own_sem
    )
    load_own.start()

    barrier = pltpu.get_barrier_semaphore()
    for o in range(1, groups):
        pl.semaphore_signal(barrier, 1, device_id=(grp_peer(o), shard), device_id_type=MESH)
    for o in range(1, shards):
        pl.semaphore_signal(barrier, 1, device_id=(grp, shard_peer(o)), device_id_type=MESH)
    pl.semaphore_wait(barrier, groups + shards - 2)

    z_copies = []
    if relay:
        outer = (grp == 0) | (grp == groups - 1)
        inner = jnp.logical_not(outer)
        mate = grp + 1 - 2 * lax.rem(grp, 2)
        near = jnp.where(outer, 3 - mate, 3 - grp)
        dests = (near, near + 1 - 2 * lax.rem(near, 2))

        def rows_of(dest, c):
            return x_ref.at[0, pl.ds(pl.multiple_of(dest * rows + c * part, 8), part), :]

        def far_copy(f):
            first = pl.multiple_of(dests[f] * rows, 8)
            return pltpu.make_async_copy(x_ref.at[0, pl.ds(first, rows), :], far.at[f], far_sem.at[f])

        def relay_copy(c, f):
            return pltpu.make_async_remote_copy(
                src_ref=rows_of(dests[f], c),
                dst_ref=passed.at[c, f],
                send_sem=r_send.at[c, f],
                recv_sem=r_recv.at[c, f],
                device_id=(mate, shard),
                device_id_type=MESH,
            )

        def mate_copy(c):
            return pltpu.make_async_remote_copy(
                src_ref=rows_of(mate, c),
                dst_ref=got[c].at[0],
                send_sem=z_send.at[c, 0],
                recv_sem=z_recv.at[c, 0],
                device_id=(mate, shard),
                device_id_type=MESH,
            )

        def packed_copies(c, f):
            return [
                pltpu.make_async_remote_copy(
                    src_ref=src.at[c, f],
                    dst_ref=dst.at[c],
                    send_sem=p_send.at[c, f, i],
                    recv_sem=p_recv.at[c, i],
                    device_id=(dests[f], shard),
                    device_id_type=MESH,
                )
                for i, (src, dst) in enumerate(((out_words, in_words), (out_peaks, in_peaks)))
            ]

        def pack_chunk(c):
            mate_copy(c).start()
            for f in range(2):
                relay_copy(c, f).wait_recv()

                def pack_pair(p, peaks, f=f):
                    at = pl.multiple_of(p * 2 * width, 2 * width)
                    pair = far[f, c * part : (c + 1) * part, pl.ds(at, 2 * width)].astype(jnp.float32)
                    pair += passed[c, f, :, pl.ds(at, 2 * width)].astype(jnp.float32)
                    words, tops = pack((pair[:, :width], pair[:, width:]))
                    for i in range(3):
                        out_words[c, f, p, i] = words[i]
                    lane = lax.broadcasted_iota(jnp.int32, (1, LANES), 1)
                    peaks = jnp.where(lane == 2 * p, tops[0], peaks)
                    return jnp.where(lane == 2 * p + 1, tops[1], peaks)

                out_peaks[c, f] = lax.fori_loop(
                    0, blocks // 2, pack_pair, jnp.zeros((1, LANES), jnp.float32), unroll=4
                )
                for copy in packed_copies(c, f):
                    copy.start()

        @pl.when(outer)
        def _():
            for c in range(chunks + 1):
                if c < chunks:
                    for f in range(2):
                        relay_copy(c, f).start()
                if c > 0:
                    mate_copy(c - 1).start()

        for f in range(2):
            far_copy(f).start()
    else:
        for c in range(chunks):
            for o in range(1, groups):
                first = pl.multiple_of(grp_peer(o) * rows + c * part, 8)
                copy = pltpu.make_async_remote_copy(
                    src_ref=x_ref.at[0, pl.ds(first, part), :],
                    dst_ref=got[c].at[o - 1],
                    send_sem=z_send.at[c, o - 1],
                    recv_sem=z_recv.at[c, o - 1],
                    device_id=(grp_peer(o), shard),
                    device_id_type=MESH,
                )
                copy.start()
                z_copies.append(copy)

    def find(j, carry):
        found, block, kind = jnp.float32(0), jnp.int32(0), jnp.int32(3)
        for b in range(blocks):
            hit = slot_ref[b] == j
            found = jnp.where(hit, 1.0, found)
            block = jnp.where(hit, joined_ref[b], block)
            kind = jnp.where(hit, (b >= QH) + (b >= QH + KVH), kind)
        source[j] = block
        taken[j] = found
        kind_of[j] = kind
        return carry

    lax.fori_loop(0, slots, find, 0)

    load_own.wait()
    if relay:
        for f in range(2):
            far_copy(f).wait()
    a_copies = []
    for step in range(chunks + 2 if relay else chunks):
        if relay and step < chunks:
            pl.when(inner)(functools.partial(pack_chunk, step))
        c = step - 2 if relay else step
        if c < 0:
            continue
        if relay:
            mate_copy(c).wait_recv()
            for copy in packed_copies(c, 0):
                copy.wait_recv()
            peaks = in_peaks[c]

            def add_pair(p, carry):
                at = pl.multiple_of(p * 2 * width, 2 * width)
                pair = own[c * part : (c + 1) * part, pl.ds(at, 2 * width)].astype(jnp.float32)
                pair += got[c][0, :, pl.ds(at, 2 * width)].astype(jnp.float32)
                tiles = unpack([in_words[c, p, i] for i in range(3)])
                lane = lax.broadcasted_iota(jnp.int32, (1, LANES), 1)
                for h in range(2):
                    peak = jnp.sum(jnp.where(lane == 2 * p + h, peaks, 0.0), axis=1, keepdims=True)
                    summed[2 * p + h] = pair[:, h * width : (h + 1) * width] + tiles[h] * peak
                return carry

            lax.fori_loop(0, blocks // 2, add_pair, 0, unroll=4)
        else:
            for o in range(1, groups):
                z_copies[c * (groups - 1) + o - 1].wait_recv()

            def add(k, carry):
                at = pl.multiple_of(k * width, width)
                total = own[c * part : (c + 1) * part, pl.ds(at, width)].astype(jnp.float32)
                for o in range(1, groups):
                    total += got[c][o - 1, :, pl.ds(at, width)].astype(jnp.float32)
                summed[k] = total
                return carry

            lax.fori_loop(0, blocks, add, 0, unroll=4)

        def slot(j, carry):
            total = summed[source[j]] * taken[j]
            ready[c][j] = total
            sq = jnp.sum((total * total).reshape(part // 8, 8, width), axis=0)
            squares[j] = sq if c == 0 else squares[j] + sq
            return carry

        lax.fori_loop(0, slots, slot, 0, unroll=4)

        if c == chunks - 1:
            lane = lax.broadcasted_iota(jnp.int32, (slots, LANES), 1)
            row = lax.broadcasted_iota(jnp.int32, (slots, LANES), 0)
            per_slot = jnp.sum(jnp.sum(squares[...], axis=1), axis=1, keepdims=True)
            shard_part[...] = jnp.sum(jnp.where(lane == row, per_slot, 0.0), axis=0, keepdims=True)
            s_copies = []
            for o in range(1, shards):
                copy = pltpu.make_async_remote_copy(
                    src_ref=shard_part,
                    dst_ref=shard_all.at[o - 1],
                    send_sem=s_send.at[o - 1],
                    recv_sem=s_recv.at[o - 1],
                    device_id=(grp, shard_peer(o)),
                    device_id_type=MESH,
                )
                copy.start()
                s_copies.append(copy)

        for o in range(1, shards):
            copy = pltpu.make_async_remote_copy(
                src_ref=ready[c].at[pl.ds(shard_peer(o) * slots_dev, slots_dev)],
                dst_ref=out_ref.at[:, shard, pl.ds(c * part, part), :],
                send_sem=a_send.at[c, o - 1],
                recv_sem=a_recv.at[c, o - 1],
                device_id=(grp, shard_peer(o)),
                device_id_type=MESH,
            )
            copy.start()
            a_copies.append(copy)
        copy = pltpu.make_async_copy(
            ready[c].at[pl.ds(shard * slots_dev, slots_dev)],
            out_ref.at[:, shard, pl.ds(c * part, part), :],
            keep_sem.at[c],
        )
        copy.start()
        a_copies.append(copy)

    total = shard_part[...]
    for o in range(1, shards):
        s_copies[o - 1].wait()
        total = total + shard_all[o - 1]
    grp_part[...] = total
    g_copies = []
    for o in range(1, groups):
        copy = pltpu.make_async_remote_copy(
            src_ref=grp_part,
            dst_ref=grp_all.at[o - 1],
            send_sem=g_send.at[o - 1],
            recv_sem=g_recv.at[o - 1],
            device_id=(grp_peer(o), shard),
            device_id_type=MESH,
        )
        copy.start()
        g_copies.append(copy)
    lane = lax.broadcasted_iota(jnp.int32, (1, LANES), 1)

    def lay(j, kinds):
        return jnp.where(lane == j, kind_of[j], kinds)

    kinds = lax.fori_loop(0, slots, lay, jnp.full((1, LANES), 3, jnp.int32))
    for o in range(1, groups):
        g_copies[o - 1].wait()
        total = total + grp_all[o - 1]
    root = jnp.sqrt(total / (D * HS))
    for i in range(slots_dev):
        head_ref[i] = jnp.sum(jnp.where(lane == shard * slots_dev + i, root, 0.0))
    for t, heads in enumerate((QH, KVH, KVH)):
        one = jnp.sum(jnp.where(kinds == t, total, 0.0), axis=1, keepdims=True)
        type_ref[t] = jnp.sum(jnp.sqrt(one / (heads * D * HS)))

    if relay:
        for c in range(chunks):
            mate_copy(c).wait_send()

        @pl.when(outer)
        def _():
            for c in range(chunks):
                for f in range(2):
                    relay_copy(c, f).wait_send()

        @pl.when(inner)
        def _():
            for c in range(chunks):
                for f in range(2):
                    for copy in packed_copies(c, f):
                        copy.wait_send()

    for copy in z_copies:
        copy.wait_send()
    for copy in a_copies:
        copy.wait()


def solution(mesh):
    groups, shards = mesh.shape["grp"], mesh.shape["shard"]

    def step(x, joined, slot):
        blocks = joined.shape[0]
        slots_dev = (blocks + shards - 1) // shards
        slots = slots_dev * shards
        rows = x.shape[1] // groups
        cols = x.shape[2]
        width = cols // blocks
        part = chunk_rows(rows)
        chunks = rows // part
        dma = pltpu.SemaphoreType.DMA
        relay = groups == 4 and part == 16 and blocks % 2 == 0 and blocks <= LANES
        relay = relay and width == LANES
        arrivals = 1 if relay else groups - 1
        return tuple(
            pl.pallas_call(
                functools.partial(kernel, groups, shards, blocks, slots_dev, chunks, relay),
                out_shape=[
                    jax.ShapeDtypeStruct((slots_dev, shards, rows, width), jnp.float32),
                    jax.ShapeDtypeStruct((slots_dev,), jnp.float32),
                    jax.ShapeDtypeStruct((3,), jnp.float32),
                ],
                in_specs=[
                    pl.BlockSpec(memory_space=pl.ANY),
                    pl.BlockSpec(memory_space=pltpu.SMEM),
                    pl.BlockSpec(memory_space=pltpu.SMEM),
                ],
                out_specs=[
                    pl.BlockSpec(memory_space=pl.ANY),
                    pl.BlockSpec(memory_space=pltpu.SMEM),
                    pl.BlockSpec(memory_space=pltpu.SMEM),
                ],
                scratch_shapes=[pltpu.VMEM((rows, cols), jnp.bfloat16)]
                + [pltpu.VMEM((arrivals, part, cols), jnp.bfloat16)] * chunks
                + [pltpu.VMEM((slots, part, width), jnp.float32)] * chunks
                + [
                    pltpu.SMEM((slots,), jnp.int32),
                    pltpu.SMEM((slots,), jnp.float32),
                    pltpu.SMEM((slots,), jnp.int32),
                    pltpu.VMEM((blocks, part, width), jnp.float32),
                    pltpu.VMEM((slots, 8, width), jnp.float32),
                    pltpu.VMEM((1, LANES), jnp.float32),
                    pltpu.VMEM((shards - 1, 1, LANES), jnp.float32),
                    pltpu.VMEM((1, LANES), jnp.float32),
                    pltpu.VMEM((groups - 1, 1, LANES), jnp.float32),
                    dma,
                    dma((chunks, arrivals)),
                    dma((chunks, arrivals)),
                    dma((chunks, shards - 1)),
                    dma((chunks, shards - 1)),
                    dma((chunks,)),
                    dma((shards - 1,)),
                    dma((shards - 1,)),
                    dma((groups - 1,)),
                    dma((groups - 1,)),
                ]
                + [
                    pltpu.VMEM((2, rows, cols), jnp.bfloat16),
                    pltpu.VMEM((chunks, 2, part, cols), jnp.bfloat16),
                    pltpu.VMEM((chunks, 2, blocks // 2, 3, 8, width), jnp.int32),
                    pltpu.VMEM((chunks, 2, 1, LANES), jnp.float32),
                    pltpu.VMEM((chunks, blocks // 2, 3, 8, width), jnp.int32),
                    pltpu.VMEM((chunks, 1, LANES), jnp.float32),
                    dma((2,)),
                    dma((chunks, 2)),
                    dma((chunks, 2)),
                    dma((chunks, 2, 2)),
                    dma((chunks, 2)),
                ]
                * relay,
                compiler_params=pltpu.CompilerParams(
                    collective_id=0,
                    has_side_effects=True,
                    vmem_limit_bytes=60 * 1024 * 1024,
                ),
            )(x, joined, slot)
        )

    return jax.shard_map(
        step,
        mesh=mesh,
        in_specs=(P("grp", "shard", None), P(), P()),
        out_specs=(P("shard", None, "grp", None), P("shard"), P()),
        check_vma=False,
    )
```

```python
import functools

import jax
import jax.numpy as jnp
from jax import lax
from jax.experimental import pallas as pl
from jax.experimental.pallas import tpu as pltpu
from jax.sharding import PartitionSpec as P

D = 4096
QH = 32
KVH = 8
HS = 128
LANES = 128
MESH = pl.DeviceIdType.MESH


def chunk_rows(rows):
    return 16 if rows % 16 == 0 else rows


QMAX = 8388600.0
TINY = 2.0**-126
AHEAD = 3


def pack(pair):
    peaks, codes = [], []
    for tile in pair:
        peak = jnp.max(jnp.abs(tile), axis=(0, 1), keepdims=True)
        shrink = jnp.where(peak > 2.0**100, 2.0**-24, 1.0)
        scale = 1.0 / jnp.maximum(peak * shrink, TINY)
        code = jnp.round(tile * shrink * scale * QMAX).astype(jnp.int32)
        peaks.append(peak)
        codes += [code[:8], code[8:]]
    a, b, c, d = codes
    words = (
        (a << 8) | (d & 255),
        (b << 8) | ((d >> 8) & 255),
        (c << 8) | ((d >> 16) & 255),
    )
    return words, peaks


def unpack(words):
    a, b, c = words
    d = (a & 255) | ((b & 255) << 8) | ((c << 24) >> 8)
    return [
        jnp.concatenate([lo.astype(jnp.float32), hi.astype(jnp.float32)], axis=0) * (1.0 / QMAX)
        for lo, hi in ((a >> 8, b >> 8), (c >> 8, d))
    ]


def kernel(groups, shards, blocks, slots_dev, chunks, relay, *refs):
    x_ref, joined_ref, slot_ref = refs[:3]
    out_ref, head_ref, type_ref = refs[3:6]
    own = refs[6]
    got = refs[7 : 7 + chunks]
    ready = refs[7 + chunks : 7 + 2 * chunks]
    rest = refs[7 + 2 * chunks :]
    if relay:
        far, passed, out_words, out_peaks, in_words, in_peaks, plain = rest[-14:-7]
        far_sem, r_send, r_recv, p_send, p_recv, d_send, d_recv = rest[-7:]
        rest = rest[:-14]
    (source, taken, kind_of, summed, squares, shard_part, shard_all, grp_part, grp_all) = rest[:9]
    (own_sem, z_send, z_recv, a_send, a_recv, keep_sem, s_send, s_recv, g_send, g_recv) = rest[9:]

    grp = lax.axis_index("grp")
    shard = lax.axis_index("shard")
    slots = slots_dev * shards
    rows = own.shape[0]
    part = rows // chunks
    width = own.shape[1] // blocks

    def grp_peer(offset):
        return lax.rem(grp + offset, groups)

    def shard_peer(offset):
        return lax.rem(shard + offset, shards)

    load_own = pltpu.make_async_copy(
        x_ref.at[0, pl.ds(pl.multiple_of(grp * rows, 8), rows), :], own, own_sem
    )
    load_own.start()

    barrier = pltpu.get_barrier_semaphore()
    for o in range(1, groups):
        pl.semaphore_signal(barrier, 1, device_id=(grp_peer(o), shard), device_id_type=MESH)
    for o in range(1, shards):
        pl.semaphore_signal(barrier, 1, device_id=(grp, shard_peer(o)), device_id_type=MESH)
    pl.semaphore_wait(barrier, groups + shards - 2)

    z_copies = []
    if relay:
        outer = (grp == 0) | (grp == groups - 1)
        inner = jnp.logical_not(outer)
        mate = grp + 1 - 2 * lax.rem(grp, 2)
        near = jnp.where(outer, 3 - mate, 3 - grp)
        dests = (near, near + 1 - 2 * lax.rem(near, 2))

        def rows_of(dest, c):
            return x_ref.at[0, pl.ds(pl.multiple_of(dest * rows + c * part, 8), part), :]

        def far_copy(f):
            first = pl.multiple_of(dests[f] * rows, 8)
            return pltpu.make_async_copy(x_ref.at[0, pl.ds(first, rows), :], far.at[f], far_sem.at[f])

        def relay_copy(c, f):
            return pltpu.make_async_remote_copy(
                src_ref=rows_of(dests[f], c),
                dst_ref=passed.at[c, f],
                send_sem=r_send.at[c, f],
                recv_sem=r_recv.at[c, f],
                device_id=(mate, shard),
                device_id_type=MESH,
            )

        def mate_copy(c):
            return pltpu.make_async_remote_copy(
                src_ref=rows_of(mate, c),
                dst_ref=got[c].at[0],
                send_sem=z_send.at[c, 0],
                recv_sem=z_recv.at[c, 0],
                device_id=(mate, shard),
                device_id_type=MESH,
            )

        def packed_copies(c, f):
            return [
                pltpu.make_async_remote_copy(
                    src_ref=src.at[c, f],
                    dst_ref=dst.at[c],
                    send_sem=p_send.at[c, f, i],
                    recv_sem=p_recv.at[c, i],
                    device_id=(dests[f], shard),
                    device_id_type=MESH,
                )
                for i, (src, dst) in enumerate(((out_words, in_words), (out_peaks, in_peaks)))
            ]

        def plain_copy(f, place):
            return pltpu.make_async_remote_copy(
                src_ref=rows_of(dests[f], 0),
                dst_ref=plain.at[place],
                send_sem=d_send.at[f],
                recv_sem=d_recv.at[place],
                device_id=(dests[f], shard),
                device_id_type=MESH,
            )

        def pack_chunk(c):
            mate_copy(c).start()
            for f in range(2):
                relay_copy(c, f).wait_recv()

                def pack_pair(p, peaks, f=f):
                    at = pl.multiple_of(p * 2 * width, 2 * width)
                    pair = far[f, c * part : (c + 1) * part, pl.ds(at, 2 * width)].astype(jnp.float32)
                    pair += passed[c, f, :, pl.ds(at, 2 * width)].astype(jnp.float32)
                    words, tops = pack((pair[:, :width], pair[:, width:]))
                    for i in range(3):
                        out_words[c, f, p, i] = words[i]
                    lane = lax.broadcasted_iota(jnp.int32, (1, LANES), 1)
                    peaks = jnp.where(lane == 2 * p, tops[0], peaks)
                    return jnp.where(lane == 2 * p + 1, tops[1], peaks)

                out_peaks[c, f] = lax.fori_loop(
                    0, blocks // 2, pack_pair, jnp.zeros((1, LANES), jnp.float32), unroll=4
                )
                for copy in packed_copies(c, f):
                    copy.start()

        for f in range(2):
            plain_copy(f, jnp.where(outer, 1, 0)).start()

        @pl.when(outer)
        def _():
            for c in range(1, chunks):
                for f in range(2):
                    relay_copy(c, f).start()
                if c >= AHEAD:
                    mate_copy(c - AHEAD).start()
            for c in range(max(chunks - AHEAD, 0), chunks):
                mate_copy(c).start()

        @pl.when(inner)
        def _():
            mate_copy(0).start()

        for f in range(2):
            far_copy(f).start()
    else:
        for c in range(chunks):
            for o in range(1, groups):
                first = pl.multiple_of(grp_peer(o) * rows + c * part, 8)
                copy = pltpu.make_async_remote_copy(
                    src_ref=x_ref.at[0, pl.ds(first, part), :],
                    dst_ref=got[c].at[o - 1],
                    send_sem=z_send.at[c, o - 1],
                    recv_sem=z_recv.at[c, o - 1],
                    device_id=(grp_peer(o), shard),
                    device_id_type=MESH,
                )
                copy.start()
                z_copies.append(copy)

    def find(j, carry):
        found, block, kind = jnp.float32(0), jnp.int32(0), jnp.int32(3)
        for b in range(blocks):
            hit = slot_ref[b] == j
            found = jnp.where(hit, 1.0, found)
            block = jnp.where(hit, joined_ref[b], block)
            kind = jnp.where(hit, (b >= QH) + (b >= QH + KVH), kind)
        source[j] = block
        taken[j] = found
        kind_of[j] = kind
        return carry

    lax.fori_loop(0, slots, find, 0)

    load_own.wait()
    if relay:
        for f in range(2):
            far_copy(f).wait()
    a_copies = []
    for step in range(chunks + AHEAD if relay else chunks):
        if relay and 0 < step < chunks:
            pl.when(inner)(functools.partial(pack_chunk, step))
        c = step - AHEAD if relay else step
        if c < 0:
            continue
        if relay:
            mate_copy(c).wait_recv()
            if c == 0:
                for place in range(2):
                    plain_copy(0, place).wait_recv()
            else:
                for copy in packed_copies(c, 0):
                    copy.wait_recv()
                peaks = in_peaks[c]

            def add_pair(p, carry):
                at = pl.multiple_of(p * 2 * width, 2 * width)
                pair = own[c * part : (c + 1) * part, pl.ds(at, 2 * width)].astype(jnp.float32)
                pair += got[c][0, :, pl.ds(at, 2 * width)].astype(jnp.float32)
                if c == 0:
                    for place in range(2):
                        pair += plain[place, :, pl.ds(at, 2 * width)].astype(jnp.float32)
                    for h in range(2):
                        summed[2 * p + h] = pair[:, h * width : (h + 1) * width]
                    return carry
                tiles = unpack([in_words[c, p, i] for i in range(3)])
                lane = lax.broadcasted_iota(jnp.int32, (1, LANES), 1)
                for h in range(2):
                    peak = jnp.sum(jnp.where(lane == 2 * p + h, peaks, 0.0), axis=1, keepdims=True)
                    summed[2 * p + h] = pair[:, h * width : (h + 1) * width] + tiles[h] * peak
                return carry

            lax.fori_loop(0, blocks // 2, add_pair, 0, unroll=4)
        else:
            for o in range(1, groups):
                z_copies[c * (groups - 1) + o - 1].wait_recv()

            def add(k, carry):
                at = pl.multiple_of(k * width, width)
                total = own[c * part : (c + 1) * part, pl.ds(at, width)].astype(jnp.float32)
                for o in range(1, groups):
                    total += got[c][o - 1, :, pl.ds(at, width)].astype(jnp.float32)
                summed[k] = total
                return carry

            lax.fori_loop(0, blocks, add, 0, unroll=4)

        def slot(j, carry):
            total = summed[source[j]] * taken[j]
            ready[c][j] = total
            sq = jnp.sum((total * total).reshape(part // 8, 8, width), axis=0)
            squares[j] = sq if c == 0 else squares[j] + sq
            return carry

        lax.fori_loop(0, slots, slot, 0, unroll=4)

        if c == chunks - 1:
            lane = lax.broadcasted_iota(jnp.int32, (slots, LANES), 1)
            row = lax.broadcasted_iota(jnp.int32, (slots, LANES), 0)
            per_slot = jnp.sum(jnp.sum(squares[...], axis=1), axis=1, keepdims=True)
            shard_part[...] = jnp.sum(jnp.where(lane == row, per_slot, 0.0), axis=0, keepdims=True)
            s_copies = []
            for o in range(1, shards):
                copy = pltpu.make_async_remote_copy(
                    src_ref=shard_part,
                    dst_ref=shard_all.at[o - 1],
                    send_sem=s_send.at[o - 1],
                    recv_sem=s_recv.at[o - 1],
                    device_id=(grp, shard_peer(o)),
                    device_id_type=MESH,
                )
                copy.start()
                s_copies.append(copy)

        for o in range(1, shards):
            copy = pltpu.make_async_remote_copy(
                src_ref=ready[c].at[pl.ds(shard_peer(o) * slots_dev, slots_dev)],
                dst_ref=out_ref.at[:, shard, pl.ds(c * part, part), :],
                send_sem=a_send.at[c, o - 1],
                recv_sem=a_recv.at[c, o - 1],
                device_id=(grp, shard_peer(o)),
                device_id_type=MESH,
            )
            copy.start()
            a_copies.append(copy)
        copy = pltpu.make_async_copy(
            ready[c].at[pl.ds(shard * slots_dev, slots_dev)],
            out_ref.at[:, shard, pl.ds(c * part, part), :],
            keep_sem.at[c],
        )
        copy.start()
        a_copies.append(copy)

    total = shard_part[...]
    for o in range(1, shards):
        s_copies[o - 1].wait()
        total = total + shard_all[o - 1]
    grp_part[...] = total
    g_copies = []
    for o in range(1, groups):
        copy = pltpu.make_async_remote_copy(
            src_ref=grp_part,
            dst_ref=grp_all.at[o - 1],
            send_sem=g_send.at[o - 1],
            recv_sem=g_recv.at[o - 1],
            device_id=(grp_peer(o), shard),
            device_id_type=MESH,
        )
        copy.start()
        g_copies.append(copy)
    lane = lax.broadcasted_iota(jnp.int32, (1, LANES), 1)

    def lay(j, kinds):
        return jnp.where(lane == j, kind_of[j], kinds)

    kinds = lax.fori_loop(0, slots, lay, jnp.full((1, LANES), 3, jnp.int32))
    for o in range(1, groups):
        g_copies[o - 1].wait()
        total = total + grp_all[o - 1]
    root = jnp.sqrt(total / (D * HS))
    for i in range(slots_dev):
        head_ref[i] = jnp.sum(jnp.where(lane == shard * slots_dev + i, root, 0.0))
    for t, heads in enumerate((QH, KVH, KVH)):
        one = jnp.sum(jnp.where(kinds == t, total, 0.0), axis=1, keepdims=True)
        type_ref[t] = jnp.sum(jnp.sqrt(one / (heads * D * HS)))

    if relay:
        for c in range(chunks):
            mate_copy(c).wait_send()
        for f in range(2):
            plain_copy(f, 0).wait_send()

        @pl.when(outer)
        def _():
            for c in range(1, chunks):
                for f in range(2):
                    relay_copy(c, f).wait_send()

        @pl.when(inner)
        def _():
            for c in range(1, chunks):
                for f in range(2):
                    for copy in packed_copies(c, f):
                        copy.wait_send()

    for copy in z_copies:
        copy.wait_send()
    for copy in a_copies:
        copy.wait()


def solution(mesh):
    groups, shards = mesh.shape["grp"], mesh.shape["shard"]

    def step(x, joined, slot):
        blocks = joined.shape[0]
        slots_dev = (blocks + shards - 1) // shards
        slots = slots_dev * shards
        rows = x.shape[1] // groups
        cols = x.shape[2]
        width = cols // blocks
        part = chunk_rows(rows)
        chunks = rows // part
        dma = pltpu.SemaphoreType.DMA
        relay = groups == 4 and part == 16 and blocks % 2 == 0 and blocks <= LANES
        relay = relay and width == LANES
        arrivals = 1 if relay else groups - 1
        return tuple(
            pl.pallas_call(
                functools.partial(kernel, groups, shards, blocks, slots_dev, chunks, relay),
                out_shape=[
                    jax.ShapeDtypeStruct((slots_dev, shards, rows, width), jnp.float32),
                    jax.ShapeDtypeStruct((slots_dev,), jnp.float32),
                    jax.ShapeDtypeStruct((3,), jnp.float32),
                ],
                in_specs=[
                    pl.BlockSpec(memory_space=pltpu.HBM),
                    pl.BlockSpec(memory_space=pltpu.SMEM),
                    pl.BlockSpec(memory_space=pltpu.SMEM),
                ],
                out_specs=[
                    pl.BlockSpec(memory_space=pl.ANY),
                    pl.BlockSpec(memory_space=pltpu.SMEM),
                    pl.BlockSpec(memory_space=pltpu.SMEM),
                ],
                scratch_shapes=[pltpu.VMEM((rows, cols), jnp.bfloat16)]
                + [pltpu.VMEM((arrivals, part, cols), jnp.bfloat16)] * chunks
                + [pltpu.VMEM((slots, part, width), jnp.float32)] * chunks
                + [
                    pltpu.SMEM((slots,), jnp.int32),
                    pltpu.SMEM((slots,), jnp.float32),
                    pltpu.SMEM((slots,), jnp.int32),
                    pltpu.VMEM((blocks, part, width), jnp.float32),
                    pltpu.VMEM((slots, 8, width), jnp.float32),
                    pltpu.VMEM((1, LANES), jnp.float32),
                    pltpu.VMEM((shards - 1, 1, LANES), jnp.float32),
                    pltpu.VMEM((1, LANES), jnp.float32),
                    pltpu.VMEM((groups - 1, 1, LANES), jnp.float32),
                    dma,
                    dma((chunks, arrivals)),
                    dma((chunks, arrivals)),
                    dma((chunks, shards - 1)),
                    dma((chunks, shards - 1)),
                    dma((chunks,)),
                    dma((shards - 1,)),
                    dma((shards - 1,)),
                    dma((groups - 1,)),
                    dma((groups - 1,)),
                ]
                + [
                    pltpu.VMEM((2, rows, cols), jnp.bfloat16),
                    pltpu.VMEM((chunks, 2, part, cols), jnp.bfloat16),
                    pltpu.VMEM((chunks, 2, blocks // 2, 3, 8, width), jnp.int32),
                    pltpu.VMEM((chunks, 2, 1, LANES), jnp.float32),
                    pltpu.VMEM((chunks, blocks // 2, 3, 8, width), jnp.int32),
                    pltpu.VMEM((chunks, 1, LANES), jnp.float32),
                    pltpu.VMEM((2, part, cols), jnp.bfloat16),
                    dma((2,)),
                    dma((chunks, 2)),
                    dma((chunks, 2)),
                    dma((chunks, 2, 2)),
                    dma((chunks, 2)),
                    dma((2,)),
                    dma((2,)),
                ]
                * relay,
                compiler_params=pltpu.CompilerParams(
                    collective_id=0,
                    has_side_effects=True,
                    vmem_limit_bytes=60 * 1024 * 1024,
                ),
            )(x, joined, slot)
        )

    return jax.shard_map(
        step,
        mesh=mesh,
        in_specs=(P("grp", "shard", None), P(), P()),
        out_specs=(P("shard", None, "grp", None), P("shard"), P()),
        check_vma=False,
    )
```
